16 devices in a mesh: rep: 1, dp: 16 (over x, y, z, core).
Axes of the slice: x: 2, y: 2, z: 2, core: 2. Of those that a mesh axis runs over, the one named last changes fastest.
Arguments:
- a: bfloat16 [16, 4, 4096, 1280], P(('rep', 'dp'))
- g: bfloat16 [16, 4, 4096, 5120], P(('rep', 'dp'))
Outputs:
- output: bfloat16 [4, 1280, 5120], P('rep')
All inputs are finite; a program needn't handle non-finite values.
Results may differ from the reference program's by a relative error of at most 0.012.
Values are sent between devices in bfloat16 or wider.
A program may use at most 2 GiB of HBM per device.

```python
import jax
import jax.numpy as jnp
from jax import lax

DEVICES = 16
MATRICES = 4
TOKENS = 4096
D = 1280
FF = 5120


def setup_inputs(seed: int = 0, part: int = 0) -> dict:
    ka, kg, ks = (jax.random.fold_in(k, part) for k in jax.random.split(jax.random.key(seed), 3))
    size = 2.0 ** jax.random.uniform(ks, (DEVICES, MATRICES, 1, 1), jnp.float32, -1.0, 1.0)
    a = jax.random.normal(ka, (DEVICES, MATRICES, TOKENS, D), jnp.float32)
    g = size * jax.random.normal(kg, (DEVICES, MATRICES, TOKENS, FF), jnp.float32) * (DEVICES * TOKENS) ** -0.5
    return {"a": a.astype(jnp.bfloat16), "g": g.astype(jnp.bfloat16)}


def reference(a, g):
    def take(so_far, one):
        return so_far + jnp.einsum("ntd,ntf->ndf", *one, preferred_element_type=jnp.float32), None

    return lax.scan(take, jnp.zeros((MATRICES, D, FF), jnp.float32), (a, g))[0].astype(jnp.bfloat16)
```

```python
import jax
import jax.numpy as jnp
from jax import lax
from jax.experimental import pallas as pl
from jax.experimental.pallas import tpu as pltpu
from jax.sharding import PartitionSpec as P

MESH = pl.DeviceIdType.MESH
W = 256
K = 256
LAG = {1: 2, 2: 5, 3: 7, 4: 9, 5: 11, 6: 14, 7: 17, 8: 19, 9: 21}
SPARE = LAG[9] - LAG[4] + 3


def kernel(shape, a, g, out, at, a_in, g_in, acc, give, take, keep1, keep2, keep3, s1, s2, s3, r1, r2, r3, whole,
           a_sem, g_sem, o_sem, d_send, d_recv, rs_send, rs_recv, ag_send, ag_recv):
    mats, tokens, rows, cols = shape
    half = rows // 2
    per = cols // W
    units = mats * per
    chunks = tokens // K
    me = lax.axis_index("dp")
    core = me % 2
    bits = ((me // 8) % 2, (me // 4) % 2, (me // 2) % 2)

    def pick(j, x, y, z):
        return jnp.where(j == 0, x, jnp.where(j == 1, y, z))

    def route(v, s):
        j = lax.rem(v + s, 3)
        bit = pick(j, *bits)
        return bit, me + pick(j, 8, 4, 2) * (1 - 2 * bit)

    other = me + 1 - 2 * core

    def remote(src, dst, send, recv, to):
        return pltpu.make_async_remote_copy(src_ref=src, dst_ref=dst, send_sem=send, recv_sem=recv,
                                            device_id={"dp": to}, device_id_type=MESH)

    def aligned(x, n):
        return pl.multiple_of(x, n)

    def g_copy(i):
        n, j = i // (per // 2), lax.rem(i, per // 2)
        return pltpu.make_async_copy(g.at[0, n, :, pl.ds(aligned(j * 2 * W, 2 * W), 2 * W)],
                                     g_in.at[lax.rem(i, 2)], g_sem.at[lax.rem(i, 2)])

    def a_copy(n, c):
        return pltpu.make_async_copy(a.at[0, n, pl.ds(aligned(c * K, K), K), :], a_in.at[lax.rem(c, 2)], a_sem.at[lax.rem(c, 2)])

    def o_copy(v):
        n, j = v // per, lax.rem(v, per)
        slot = lax.rem(v, SPARE)
        return pltpu.make_async_copy(whole.at[slot], out.at[n, :, pl.ds(aligned(j * W, W), W)], o_sem.at[lax.rem(v, 3)])

    def flip(n, c):
        at[lax.rem(n, 2), :, pl.ds(aligned(c * K, K), K)] = a_in[lax.rem(c, 2)].T

    def swap(i):
        return remote(give, take.at[lax.rem(i, 3)], d_send.at[0], d_recv.at[lax.rem(i, 3)], other)

    def scatter(v, s):
        src, dst = ((s1, r1), (s2, r2), (s3, r3))[s]
        _, to = route(v, s)
        q = lax.rem(v, 6)
        return remote(src.at[lax.rem(v, 3)], dst.at[q], rs_send.at[s, lax.rem(v, 3)], rs_recv.at[s, q], to)

    def start_of(v, s):
        row, size = core * half, half
        for k in range(s):
            size //= 2
            row = row + route(v, k)[0] * size
        return row, size

    def gather(v, s):
        row, size = start_of(v, s + 1)
        _, to = route(v, s)
        q = lax.rem(v, 6)
        ref = whole.at[lax.rem(v, SPARE), pl.ds(aligned(row, rows // 16), size), :]
        return remote(ref, ref, ag_send.at[s, q], ag_recv.at[s, q], to)

    def share(v):
        q = lax.rem(v, 6)
        ref = whole.at[lax.rem(v, SPARE), pl.ds(aligned(core * half, half), half), :]
        return remote(ref, ref, ag_send.at[3, q], ag_recv.at[3, q], other)

    def add(v, s, mine, got, keep, send):
        bit, _ = route(v, s)
        n = got.shape[0] // 2
        yes, no = pl.ds(aligned(bit * n, n), n), pl.ds(aligned((1 - bit) * n, n), n)
        q = lax.rem(v, 3)
        send[q] = (mine[no, :] + got[no, :].astype(jnp.float32)).astype(jnp.bfloat16)
        keep[q] = mine[yes, :] + got[yes, :].astype(jnp.float32)

    def stages(t, h):
        def when(k, f):
            v = t - LAG[k]
            pl.when((v >= 0) & (v < units))(lambda: f(v))

        def nine(v):
            o_copy(v).wait()

        def eight(v):
            share(v).wait()
            o_copy(v).start()

        def seven(v):
            gather(v, 0).wait()
            share(v).start()

        def six(v):
            gather(v, 1).wait()
            gather(v, 0).start()

        def five(v):
            gather(v, 2).wait()
            gather(v, 1).start()

        def four(v):
            scatter(v, 2).wait()
            row, size = start_of(v, 3)
            done = keep3[lax.rem(v, 3)] + r3[lax.rem(v, 6)].astype(jnp.float32)
            whole[lax.rem(v, SPARE), pl.ds(aligned(row, rows // 16), size), :] = done.astype(jnp.bfloat16)
            gather(v, 2).start()

        def three(v):
            scatter(v, 1).wait()
            add(v, 2, keep2.at[lax.rem(v, 3)], r2.at[lax.rem(v, 6)], keep3, s3)
            scatter(v, 2).start()

        def two(v):
            scatter(v, 0).wait()
            add(v, 1, keep1.at[lax.rem(v, 3)], r1.at[lax.rem(v, 6)], keep2, s2)
            scatter(v, 1).start()

        def one(v):
            p = (h - LAG[1]) % 2
            i = v // 2
            if p == 0:
                swap(i).wait()
            c = slice(p * W, (p + 1) * W)
            add(v, 0, acc.at[:, c], take.at[lax.rem(i, 3), :, c], keep1, s1)
            scatter(v, 0).start()

        for k, f in ((9, nine), (8, eight), (7, seven), (6, six), (5, five), (4, four), (3, three), (2, two), (1, one)):
            when(k, f)

    g_copy(0).start()
    a_copy(0, 0).start()
    barrier = pltpu.get_barrier_semaphore()
    for b, bit in ((8, bits[0]), (4, bits[1]), (2, bits[2]), (1, core)):
        pl.semaphore_signal(barrier, inc=1, device_id={"dp": me + b * (1 - 2 * bit)}, device_id_type=MESH)
    pl.semaphore_wait(barrier, 4)

    def first(c, _):
        a_copy(0, c).wait()

        @pl.when(c + 1 < chunks)
        def _():
            a_copy(0, c + 1).start()
        flip(0, c)
        return 0

    lax.fori_loop(0, chunks, first, 0)

    def pair(i, _):
        n = (2 * i) // per
        for h in range(2):
            t = 2 * i + h
            c = lax.rem(t, per)
            ahead = (t < units - per) & (c < chunks)

            @pl.when(ahead)
            def _():
                a_copy(n + 1, c).start()

            stages(t, h)

            @pl.when(t < units)
            def _():
                if h == 0:
                    g_copy(i).wait()

                    @pl.when(i + 1 < units // 2)
                    def _():
                        g_copy(i + 1).start()
                side = core if h else 1 - core
                block = jnp.dot(at[lax.rem(n, 2), pl.ds(aligned(side * half, half), half), :], g_in[lax.rem(i, 2)],
                                preferred_element_type=jnp.float32)
                if h == 0:
                    give[...] = block.astype(jnp.bfloat16)
                    swap(i).start()
                else:
                    acc[...] = block

            @pl.when(ahead)
            def _():
                a_copy(n + 1, c).wait()
                flip(n + 1, c)
        return 0

    lax.fori_loop(0, (units + LAG[9] + 1 + 1) // 2, pair, 0)


def solution(mesh):
    def step(a, g):
        _, mats, tokens, rows = a.shape
        cols = g.shape[3]
        half = rows // 2
        bf, f32 = jnp.bfloat16, jnp.float32
        dma = pltpu.SemaphoreType.DMA
        return pl.pallas_call(
            lambda *refs: kernel((mats, tokens, rows, cols), *refs),
            out_shape=jax.ShapeDtypeStruct((mats, rows, cols), bf),
            in_specs=[pl.BlockSpec(memory_space=pl.ANY)] * 2,
            out_specs=pl.BlockSpec(memory_space=pl.ANY),
            scratch_shapes=[
                pltpu.VMEM((2, rows, tokens), bf),
                pltpu.VMEM((2, K, rows), bf),
                pltpu.VMEM((2, tokens, 2 * W), bf),
                pltpu.VMEM((half, 2 * W), f32),
                pltpu.VMEM((half, 2 * W), bf),
                pltpu.VMEM((3, half, 2 * W), bf),
                *[pltpu.VMEM((3, half // d, W), f32) for d in (2, 4, 8)],
                *[pltpu.VMEM((3, half // d, W), bf) for d in (2, 4, 8)],
                *[pltpu.VMEM((6, half // d, W), bf) for d in (2, 4, 8)],
                pltpu.VMEM((SPARE, rows, W), bf),
                dma((2,)), dma((2,)), dma((3,)), dma((1,)), dma((3,)),
                dma((3, 3)), dma((3, 6)), dma((4, 6)), dma((4, 6)),
            ],
            compiler_params=pltpu.CompilerParams(collective_id=0, has_side_effects=True, vmem_limit_bytes=63 * 2**20),
        )(a, g)

    return jax.shard_map(step, mesh=mesh, in_specs=(P(("rep", "dp")), P(("rep", "dp"))), out_specs=P("rep"), check_vma=False)
```

```python
import jax
import jax.numpy as jnp
from jax import lax
from jax.experimental import pallas as pl
from jax.experimental.pallas import tpu as pltpu
from jax.sharding import PartitionSpec as P

MESH = pl.DeviceIdType.MESH
W = 256
K = 256
LAG = {1: 2, 2: 4, 3: 6, 4: 8, 5: 10, 6: 13, 7: 16, 8: 18, 9: 20}
LANES = 16
SPARE = 2 * LANES
COLUMNS, UNITS, BLOCKS = 2, 3, 5
ROWS = 4

def kernel(shape, a, g, out, pool, a_in, acc, give, take, keep1, keep2, keep3, s1, s2, s3, r1, r2, r3,
           a_sem, g_sem, o_sem, b_sem, d_send, d_recv, rs_send, rs_recv, ag_send, ag_recv):
    mats, tokens, rows, cols = shape
    half = rows // 2
    per = cols // W
    units = mats * per
    chunks = tokens // K
    early = units - SPARE
    deep = tokens // 4
    me = lax.axis_index("dp")
    core = me % 2
    bits = ((me // 8) % 2, (me // 4) % 2, (me // 2) % 2)

    def pick(j, x, y, z):
        return jnp.where(j == 0, x, jnp.where(j == 1, y, z))

    def route(v, s):
        j = lax.rem(v + s, 3)
        bit = pick(j, *bits)
        return bit, me + pick(j, 8, 4, 2) * (1 - 2 * bit)

    other = me + 1 - 2 * core

    def remote(src, dst, send, recv, to):
        return pltpu.make_async_remote_copy(src_ref=src, dst_ref=dst, send_sem=send, recv_sem=recv,
                                            device_id={"dp": to}, device_id_type=MESH)

    def aligned(x, n):
        return pl.multiple_of(x, n)

    def piece(i, q):
        return COLUMNS, pl.ds(0, deep), pl.ds(aligned((4 * lax.rem(i, 2) + q) * 2 * W, 2 * W), 2 * W)

    def g_copies(i):
        n, j = i // (per // 2), lax.rem(i, per // 2)
        return [pltpu.make_async_copy(g.at[0, n, pl.ds(q * deep, deep), pl.ds(aligned(j * 2 * W, 2 * W), 2 * W)],
                                      pool.at[piece(i, q)], g_sem.at[lax.rem(i, 2), q]) for q in range(4)]

    def a_copy(n, c):
        return pltpu.make_async_copy(a.at[0, n, pl.ds(aligned(c * K, K), K), :], a_in.at[lax.rem(c, 4)], a_sem.at[lax.rem(c, 4)])

    def spot(v, row, size):
        r = lax.rem(v, SPARE)
        return UNITS + r // LANES, pl.ds(row, size), pl.ds(aligned(lax.rem(r, LANES) * W, W), W)

    def home(v):
        n, j = v // per, lax.rem(v, per)
        return out.at[n, :, pl.ds(aligned(j * W, W), W)]

    def o_copy(v):
        return pltpu.make_async_copy(pool.at[spot(v, 0, rows)], home(v), o_sem.at[lax.rem(v, 3)])

    def back(f, q):
        return pltpu.make_async_copy(home(f), pool.at[f // LANES, :, pl.ds(aligned(lax.rem(f, LANES) * W, W), W)], b_sem.at[q])

    def fetch(t, act):
        f = t - (units - per)
        pl.when((f >= 0) & (f < LANES))(lambda: act(back(f, 0)))
        for q in range(2):
            f = LANES + 2 * (t - units) + q
            pl.when((f >= LANES) & (f < early))(lambda f=f, q=q: act(back(f, q)))

    def flip(n, c):
        pool[lax.rem(n, 2), :, pl.ds(aligned(c * K, K), K)] = a_in[lax.rem(c, 4)].T

    def swap(i):
        return remote(give, take.at[lax.rem(i, 3)], d_send.at[0], d_recv.at[lax.rem(i, 3)], other)

    def scatter(v, s):
        src, dst = ((s1, r1), (s2, r2), (s3, r3))[s]
        _, to = route(v, s)
        q = lax.rem(v, 6)
        return remote(src.at[lax.rem(v, 3)], dst.at[q], rs_send.at[s, lax.rem(v, 3)], rs_recv.at[s, q], to)

    def start_of(v, s):
        row, size = core * half, half
        for k in range(s):
            size //= 2
            row = row + route(v, k)[0] * size
        return row, size

    def gather(v, s):
        row, size = start_of(v, s + 1)
        _, to = route(v, s)
        q = lax.rem(v, 6)
        ref = pool.at[spot(v, aligned(row, rows // 16), size)]
        return remote(ref, ref, ag_send.at[s, q], ag_recv.at[s, q], to)

    def share(v):
        q = lax.rem(v, 6)
        ref = pool.at[spot(v, aligned(core * half, half), half)]
        return remote(ref, ref, ag_send.at[3, q], ag_recv.at[3, q], other)

    def add(v, s, mine, got, keep, send):
        bit, _ = route(v, s)
        n = got.shape[0] // 2
        yes, no = pl.ds(aligned(bit * n, n), n), pl.ds(aligned((1 - bit) * n, n), n)
        q = lax.rem(v, 3)
        send[q] = (mine[no, :] + got[no, :].astype(jnp.float32)).astype(jnp.bfloat16)
        keep[q] = mine[yes, :] + got[yes, :].astype(jnp.float32)

    def stages(t, h):
        def when(k, f):
            v = t - LAG[k]
            pl.when((v >= 0) & (v < units))(lambda: f(v))

        def nine(v):
            pl.when(v < early)(lambda: o_copy(v).wait())

        def eight(v):
            share(v).wait()
            pl.when(v < early)(lambda: o_copy(v).start())

        def seven(v):
            gather(v, 0).wait()
            share(v).start()

        def six(v):
            gather(v, 1).wait()
            gather(v, 0).start()

        def five(v):
            gather(v, 2).wait()
            gather(v, 1).start()

        def four(v):
            scatter(v, 2).wait()
            row, size = start_of(v, 3)
            done = keep3[lax.rem(v, 3)] + r3[lax.rem(v, 6)].astype(jnp.float32)
            pool[spot(v, aligned(row, rows // 16), size)] = done.astype(jnp.bfloat16)
            gather(v, 2).start()

        def three(v):
            scatter(v, 1).wait()
            add(v, 2, keep2.at[lax.rem(v, 3)], r2.at[lax.rem(v, 6)], keep3, s3)
            scatter(v, 2).start()

        def two(v):
            scatter(v, 0).wait()
            add(v, 1, keep1.at[lax.rem(v, 3)], r1.at[lax.rem(v, 6)], keep2, s2)
            scatter(v, 1).start()

        def one(v):
            p = (h - LAG[1]) % 2
            i = v // 2
            if p == 0:
                swap(i).wait()
            c = slice(p * W, (p + 1) * W)
            add(v, 0, acc.at[:, c], take.at[lax.rem(i, 3), :, c], keep1, s1)
            scatter(v, 0).start()

        for k, f in ((9, nine), (8, eight), (7, seven), (6, six), (5, five), (4, four), (3, three), (2, two), (1, one)):
            when(k, f)

    for c in range(3):
        a_copy(0, c).start()
    for c in g_copies(0):
        c.start()
    barrier = pltpu.get_barrier_semaphore()
    for b, bit in ((8, bits[0]), (4, bits[1]), (2, bits[2]), (1, core)):
        pl.semaphore_signal(barrier, inc=1, device_id={"dp": me + b * (1 - 2 * bit)}, device_id_type=MESH)
    pl.semaphore_wait(barrier, 4)

    def first(c, _):
        a_copy(0, c).wait()

        @pl.when(c + 3 < chunks)
        def _():
            a_copy(0, c + 3).start()
        flip(0, c)
        return 0

    lax.fori_loop(0, chunks, first, 0)

    def pair(i, _):
        n = (2 * i) // per
        for h in range(2):
            t = 2 * i + h
            c = lax.rem(t, per)
            ahead = (t < units - per) & (c < chunks)

            @pl.when(ahead)
            def _():
                a_copy(n + 1, c).start()

            fetch(t - 1, lambda c: c.wait())
            stages(t, h)
            fetch(t, lambda c: c.start())

            @pl.when(t < units)
            def _():
                if h == 0:
                    for c_ in g_copies(i):
                        c_.wait()

                    @pl.when(i + 1 < units // 2)
                    def _():
                        for c_ in g_copies(i + 1):
                            c_.start()
                side = core if h else 1 - core
                mine = lax.rem(n, 2), pl.ds(aligned(side * half, half), half)
                block = sum(jnp.dot(pool[(*mine, pl.ds(q * deep, deep))], pool[piece(i, q)], preferred_element_type=jnp.float32)
                            for q in range(4))
                if h == 0:
                    give[...] = block.astype(jnp.bfloat16)
                    swap(i).start()
                else:
                    acc[...] = block

            @pl.when(ahead)
            def _():
                a_copy(n + 1, c).wait()
                flip(n + 1, c)
        return 0

    lax.fori_loop(0, (units + LAG[9] + 1 + 1) // 2, pair, 0)


def settle(shape, pool, out, sem):
    mats, rows, cols = shape
    per = cols // W
    units = mats * per
    copies, f = [], 0
    while f < units:
        n = min(LANES - f % LANES, per - f % per)
        b = f // LANES if f < units - SPARE else UNITS + f % SPARE // LANES
        for r in range(0, rows, rows // ROWS):
            part = pl.ds(r, rows // ROWS)
            copies.append(pltpu.make_async_copy(pool.at[b, part, pl.ds(f % LANES * W, n * W)],
                                                out.at[f // per, part, pl.ds(f % per * W, n * W)], sem.at[len(copies)]))
        f += n
    for c in copies:
        c.start()
    for c in copies:
        c.wait()


def solution(mesh):
    def step(a, g):
        _, mats, tokens, rows = a.shape
        cols = g.shape[3]
        half = rows // 2
        bf, f32 = jnp.bfloat16, jnp.float32
        dma = pltpu.SemaphoreType.DMA
        _, pool = pl.pallas_call(
            lambda *refs: kernel((mats, tokens, rows, cols), *refs),
            out_shape=(jax.ShapeDtypeStruct((mats, rows, cols), bf), pltpu.VMEM((BLOCKS, rows, LANES * W), bf)),
            in_specs=[pl.BlockSpec(memory_space=pl.ANY)] * 2,
            out_specs=(pl.BlockSpec(memory_space=pl.ANY), pl.BlockSpec(memory_space=pltpu.VMEM)),
            scratch_shapes=[
                pltpu.VMEM((4, K, rows), bf),
                pltpu.VMEM((half, 2 * W), f32),
                pltpu.VMEM((half, 2 * W), bf),
                pltpu.VMEM((3, half, 2 * W), bf),
                *[pltpu.VMEM((3, half // d, W), f32) for d in (2, 4, 8)],
                *[pltpu.VMEM((3, half // d, W), bf) for d in (2, 4, 8)],
                *[pltpu.VMEM((6, half // d, W), bf) for d in (2, 4, 8)],
                dma((4,)), dma((2, 4)), dma((3,)), dma((2,)), dma((1,)), dma((3,)),
                dma((3, 3)), dma((3, 6)), dma((4, 6)), dma((4, 6)),
            ],
            compiler_params=pltpu.CompilerParams(collective_id=0, has_side_effects=True, vmem_limit_bytes=14417920),
        )(a, g)
        return pl.pallas_call(
            lambda *refs: settle((mats, rows, cols), *refs),
            out_shape=jax.ShapeDtypeStruct((mats, rows, cols), bf),
            in_specs=[pl.BlockSpec(memory_space=pltpu.VMEM)],
            out_specs=pl.BlockSpec(memory_space=pl.ANY),
            scratch_shapes=[dma((8 * ROWS,))],
            compiler_params=pltpu.CompilerParams(vmem_limit_bytes=2**20),
        )(pool)

    return jax.shard_map(step, mesh=mesh, in_specs=(P(("rep", "dp")), P(("rep", "dp"))), out_specs=P("rep"), check_vma=False)
```

```python
import jax
import jax.numpy as jnp
from jax import lax
from jax.experimental import pallas as pl
from jax.experimental.pallas import tpu as pltpu
from jax.sharding import PartitionSpec as P

MESH = pl.DeviceIdType.MESH
W = 256
K = 256
LAG = {1: 2, 2: 4, 3: 6, 4: 8, 5: 10, 6: 13, 7: 16, 8: 18, 9: 20}
LANES = 16
SPARE = 2 * LANES
COLUMNS, UNITS, BLOCKS = 2, 3, 5
ROWS = 4

def kernel(shape, a, g, out, pool, a_in, acc, give, take, keep1, keep2, keep3, s1, s2, s3, r1, r2, r3,
           a_sem, g_sem, o_sem, b_sem, d_send, d_recv, rs_send, rs_recv, ag_send, ag_recv):
    mats, tokens, rows, cols = shape
    half = rows // 2
    per = cols // W
    units = mats * per
    chunks = tokens // K
    early = units - SPARE
    deep = tokens // 4
    me = lax.axis_index("dp")
    core = me % 2
    bits = ((me // 8) % 2, (me // 4) % 2, (me // 2) % 2)

    def pick(j, x, y, z):
        return jnp.where(j == 0, x, jnp.where(j == 1, y, z))

    def route(v, s):
        j = lax.rem(v + s, 3)
        bit = pick(j, *bits)
        return bit, me + pick(j, 8, 4, 2) * (1 - 2 * bit)

    other = me + 1 - 2 * core

    def remote(src, dst, send, recv, to):
        return pltpu.make_async_remote_copy(src_ref=src, dst_ref=dst, send_sem=send, recv_sem=recv,
                                            device_id={"dp": to}, device_id_type=MESH)

    def aligned(x, n):
        return pl.multiple_of(x, n)

    def piece(i, q):
        return COLUMNS, pl.ds(0, deep), pl.ds(aligned((4 * lax.rem(i, 2) + q) * 2 * W, 2 * W), 2 * W)

    def g_copies(i):
        n, j = i // (per // 2), lax.rem(i, per // 2)
        return [pltpu.make_async_copy(g.at[0, n, pl.ds(q * deep, deep), pl.ds(aligned(j * 2 * W, 2 * W), 2 * W)],
                                      pool.at[piece(i, q)], g_sem.at[lax.rem(i, 2), q]) for q in range(4)]

    def a_copy(n, c):
        return pltpu.make_async_copy(a.at[0, n, pl.ds(aligned(c * K, K), K), :], a_in.at[lax.rem(c, 4)], a_sem.at[lax.rem(c, 4)])

    def spot(v, row, size):
        r = lax.rem(v, SPARE)
        return UNITS + r // LANES, pl.ds(row, size), pl.ds(aligned(lax.rem(r, LANES) * W, W), W)

    def home(v):
        n, j = v // per, lax.rem(v, per)
        return out.at[n, :, pl.ds(aligned(j * W, W), W)]

    def o_copy(v):
        return pltpu.make_async_copy(pool.at[spot(v, 0, rows)], home(v), o_sem.at[lax.rem(v, 3)])

    def back(f, q):
        return pltpu.make_async_copy(home(f), pool.at[f // LANES, :, pl.ds(aligned(lax.rem(f, LANES) * W, W), W)], b_sem.at[q])

    def fetch(t, act):
        sem = 2 * lax.rem(t, 4)
        f = t - (units - per)
        pl.when((f >= 0) & (f < LANES))(lambda: act(back(f, sem)))
        for q in range(2):
            f = LANES + 2 * (t - units) + q
            pl.when((f >= LANES) & (f < early))(lambda f=f, q=q: act(back(f, sem + q)))

    def flip(n, c):
        pool[lax.rem(n, 2), :, pl.ds(aligned(c * K, K), K)] = a_in[lax.rem(c, 4)].T

    def swap(i):
        return remote(give, take.at[lax.rem(i, 3)], d_send.at[0], d_recv.at[lax.rem(i, 3)], other)

    def scatter(v, s):
        src, dst = ((s1, r1), (s2, r2), (s3, r3))[s]
        _, to = route(v, s)
        q = lax.rem(v, 6)
        return remote(src.at[lax.rem(v, 3)], dst.at[q], rs_send.at[s, lax.rem(v, 3)], rs_recv.at[s, q], to)

    def start_of(v, s):
        row, size = core * half, half
        for k in range(s):
            size //= 2
            row = row + route(v, k)[0] * size
        return row, size

    def gather(v, s):
        row, size = start_of(v, s + 1)
        _, to = route(v, s)
        q = lax.rem(v, 12)
        ref = pool.at[spot(v, aligned(row, rows // 16), size)]
        return remote(ref, ref, ag_send.at[s, q], ag_recv.at[s, q], to)

    def share(v):
        q = lax.rem(v, 12)
        ref = pool.at[spot(v, aligned(core * half, half), half)]
        return remote(ref, ref, ag_send.at[3, q], ag_recv.at[3, q], other)

    def add(v, s, mine, got, keep, send):
        bit, _ = route(v, s)
        n = got.shape[0] // 2
        yes, no = pl.ds(aligned(bit * n, n), n), pl.ds(aligned((1 - bit) * n, n), n)
        q = lax.rem(v, 3)
        send[q] = (mine[no, :] + got[no, :].astype(jnp.float32)).astype(jnp.bfloat16)
        keep[q] = mine[yes, :] + got[yes, :].astype(jnp.float32)

    def stages(t, h):
        def when(k, f):
            v = t - LAG[k]
            pl.when((v >= 0) & (v < units))(lambda: f(v))

        def nine(v):
            pl.when(v < early)(lambda: o_copy(v).wait())

        def eight(v):
            share(v).wait()
            pl.when(v < early)(lambda: o_copy(v).start())

        def seven(v):
            gather(v, 0).wait()
            share(v).start()

        def six(v):
            gather(v, 1).wait()
            gather(v, 0).start()

        def five(v):
            gather(v, 2).wait()
            gather(v, 1).start()

        def four(v):
            scatter(v, 2).wait()
            row, size = start_of(v, 3)
            done = keep3[lax.rem(v, 3)] + r3[lax.rem(v, 6)].astype(jnp.float32)
            pool[spot(v, aligned(row, rows // 16), size)] = done.astype(jnp.bfloat16)
            gather(v, 2).start()

        def three(v):
            scatter(v, 1).wait()
            add(v, 2, keep2.at[lax.rem(v, 3)], r2.at[lax.rem(v, 6)], keep3, s3)
            scatter(v, 2).start()

        def two(v):
            scatter(v, 0).wait()
            add(v, 1, keep1.at[lax.rem(v, 3)], r1.at[lax.rem(v, 6)], keep2, s2)
            scatter(v, 1).start()

        def one(v):
            p = (h - LAG[1]) % 2
            i = v // 2
            if p == 0:
                swap(i).wait()
            c = slice(p * W, (p + 1) * W)
            add(v, 0, acc.at[:, c], take.at[lax.rem(i, 3), :, c], keep1, s1)
            scatter(v, 0).start()

        for k, f in enumerate((one, two, three, four, five, six, seven, eight, nine), 1):
            when(k, f)

    for c in range(3):
        a_copy(0, c).start()
    for c in g_copies(0):
        c.start()
    barrier = pltpu.get_barrier_semaphore()
    for b, bit in ((8, bits[0]), (4, bits[1]), (2, bits[2]), (1, core)):
        pl.semaphore_signal(barrier, inc=1, device_id={"dp": me + b * (1 - 2 * bit)}, device_id_type=MESH)
    pl.semaphore_wait(barrier, 4)

    def first(c, _):
        a_copy(0, c).wait()

        @pl.when(c + 3 < chunks)
        def _():
            a_copy(0, c + 3).start()
        flip(0, c)
        return 0

    lax.fori_loop(0, chunks, first, 0)

    def pair(i, _):
        n = (2 * i) // per
        for h in range(2):
            t = 2 * i + h
            c = 2 * (lax.rem(t, per) - (per - chunks // 2))
            ahead = (t < units - per) & (c >= 0)

            @pl.when(ahead)
            def _():
                a_copy(n + 1, c).start()
                a_copy(n + 1, c + 1).start()

            stages(t, h)
            fetch(t - 3, lambda c: c.wait())
            fetch(t, lambda c: c.start())

            @pl.when(t < units)
            def _():
                if h == 0:
                    for c_ in g_copies(i):
                        c_.wait()

                    @pl.when(i + 1 < units // 2)
                    def _():
                        for c_ in g_copies(i + 1):
                            c_.start()
                side = core if h else 1 - core
                mine = lax.rem(n, 2), pl.ds(aligned(side * half, half), half)
                block = sum(jnp.dot(pool[(*mine, pl.ds(q * deep, deep))], pool[piece(i, q)], preferred_element_type=jnp.float32)
                            for q in range(4))
                if h == 0:
                    give[...] = block.astype(jnp.bfloat16)
                    swap(i).start()
                else:
                    acc[...] = block

            @pl.when(ahead)
            def _():
                for q in range(2):
                    a_copy(n + 1, c + q).wait()
                    flip(n + 1, c + q)
        return 0

    lax.fori_loop(0, (units + LAG[9] + 1 + 1) // 2, pair, 0)


def settle(shape, pool, out, sem):
    mats, rows, cols = shape
    per = cols // W
    units = mats * per
    copies, f = [], 0
    while f < units:
        n = min(LANES - f % LANES, per - f % per)
        b = f // LANES if f < units - SPARE else UNITS + f % SPARE // LANES
        for r in range(0, rows, rows // ROWS):
            part = pl.ds(r, rows // ROWS)
            copies.append(pltpu.make_async_copy(pool.at[b, part, pl.ds(f % LANES * W, n * W)],
                                                out.at[f // per, part, pl.ds(f % per * W, n * W)], sem.at[len(copies)]))
        f += n
    for c in copies:
        c.start()
    for c in copies:
        c.wait()


def solution(mesh):
    def step(a, g):
        _, mats, tokens, rows = a.shape
        cols = g.shape[3]
        half = rows // 2
        bf, f32 = jnp.bfloat16, jnp.float32
        dma = pltpu.SemaphoreType.DMA
        _, pool = pl.pallas_call(
            lambda *refs: kernel((mats, tokens, rows, cols), *refs),
            out_shape=(jax.ShapeDtypeStruct((mats, rows, cols), bf), pltpu.VMEM((BLOCKS, rows, LANES * W), bf)),
            in_specs=[pl.BlockSpec(memory_space=pl.ANY)] * 2,
            out_specs=(pl.BlockSpec(memory_space=pl.ANY), pl.BlockSpec(memory_space=pltpu.VMEM)),
            scratch_shapes=[
                pltpu.VMEM((4, K, rows), bf),
                pltpu.VMEM((half, 2 * W), f32),
                pltpu.VMEM((half, 2 * W), bf),
                pltpu.VMEM((3, half, 2 * W), bf),
                *[pltpu.VMEM((3, half // d, W), f32) for d in (2, 4, 8)],
                *[pltpu.VMEM((3, half // d, W), bf) for d in (2, 4, 8)],
                *[pltpu.VMEM((6, half // d, W), bf) for d in (2, 4, 8)],
                dma((4,)), dma((2, 4)), dma((3,)), dma((8,)), dma((1,)), dma((3,)),
                dma((3, 3)), dma((3, 6)), dma((4, 12)), dma((4, 12)),
            ],
            compiler_params=pltpu.CompilerParams(collective_id=0, has_side_effects=True, vmem_limit_bytes=14417920),
        )(a, g)
        return pl.pallas_call(
            lambda *refs: settle((mats, rows, cols), *refs),
            out_shape=jax.ShapeDtypeStruct((mats, rows, cols), bf),
            in_specs=[pl.BlockSpec(memory_space=pltpu.VMEM)],
            out_specs=pl.BlockSpec(memory_space=pl.ANY),
            scratch_shapes=[dma((8 * ROWS,))],
            compiler_params=pltpu.CompilerParams(vmem_limit_bytes=2**20),
        )(pool)

    return jax.shard_map(step, mesh=mesh, in_specs=(P(("rep", "dp")), P(("rep", "dp"))), out_specs=P("rep"), check_vma=False)
```

```python
import jax
import jax.numpy as jnp
from jax import lax
from jax.experimental import pallas as pl
from jax.experimental.pallas import tpu as pltpu
from jax.sharding import PartitionSpec as P

MESH = pl.DeviceIdType.MESH
W = 256
K = 256
LAG = {1: 2, 2: 4, 3: 6, 4: 8, 5: 10, 6: 13, 7: 17, 8: 19, 9: 21}
LANES = 16
SPARE = 2 * LANES
COLUMNS, UNITS, BLOCKS = 2, 3, 5
ROWS = 4

def kernel(shape, a, g, out, pool, a_in, acc, give, take, keep1, keep2, keep3, s1, s2, s3, r1, r2, r3,
           a_sem, f_sem, g_sem, o_sem, b_sem, d_send, d_recv, rs_send, rs_recv, ag_send, ag_recv):
    mats, tokens, rows, cols = shape
    half = rows // 2
    per = cols // W
    units = mats * per
    chunks = tokens // K
    early = units - SPARE
    deep = tokens // 4
    me = lax.axis_index("dp")
    core = me % 2
    bits = ((me // 8) % 2, (me // 4) % 2, (me // 2) % 2)

    def pick(j, x, y, z):
        return jnp.where(j == 0, x, jnp.where(j == 1, y, z))

    def route(v, s):
        j = lax.rem(v + s, 3)
        bit = pick(j, *bits)
        return bit, me + pick(j, 8, 4, 2) * (1 - 2 * bit)

    other = me + 1 - 2 * core

    def remote(src, dst, send, recv, to):
        return pltpu.make_async_remote_copy(src_ref=src, dst_ref=dst, send_sem=send, recv_sem=recv,
                                            device_id={"dp": to}, device_id_type=MESH)

    def aligned(x, n):
        return pl.multiple_of(x, n)

    def piece(i, q):
        return COLUMNS, pl.ds(0, deep), pl.ds(aligned((4 * lax.rem(i, 2) + q) * 2 * W, 2 * W), 2 * W)

    def g_copies(i):
        n, j = i // (per // 2), lax.rem(i, per // 2)
        return [pltpu.make_async_copy(g.at[0, n, pl.ds(q * deep, deep), pl.ds(aligned(j * 2 * W, 2 * W), 2 * W)],
                                      pool.at[piece(i, q)], g_sem.at[lax.rem(i, 2), q]) for q in range(4)]

    def a_copy(n, c):
        return pltpu.make_async_copy(a.at[0, n, pl.ds(aligned(c * K, K), K), :], a_in.at[lax.rem(c, 4)], a_sem.at[lax.rem(c, 4)])

    def spot(v, row, size):
        r = lax.rem(v, SPARE)
        return UNITS + r // LANES, pl.ds(row, size), pl.ds(aligned(lax.rem(r, LANES) * W, W), W)

    def home(v):
        n, j = v // per, lax.rem(v, per)
        return out.at[n, :, pl.ds(aligned(j * W, W), W)]

    def o_copy(v):
        return pltpu.make_async_copy(pool.at[spot(v, 0, rows)], home(v), o_sem.at[lax.rem(v, 3)])

    def back(f, q):
        return pltpu.make_async_copy(home(f), pool.at[f // LANES, :, pl.ds(aligned(lax.rem(f, LANES) * W, W), W)], b_sem.at[q])

    def fetch(t, act):
        sem = 2 * lax.rem(t, 4)
        f = t - (units - per)
        pl.when((f >= 0) & (f < LANES))(lambda: act(back(f, sem)))
        for q in range(2):
            f = LANES + 2 * (t - units) + q
            pl.when((f >= LANES) & (f < early))(lambda f=f, q=q: act(back(f, sem + q)))

    def lobby(c):
        tall, wide = rows // K, LANES * W // rows
        return (UNITS + c // (tall * wide), pl.ds(aligned(lax.rem(c, tall) * K, K), K),
                pl.ds(aligned(lax.rem(c // tall, wide) * rows, rows), rows))

    def a_first(c):
        return pltpu.make_async_copy(a.at[0, 0, pl.ds(aligned(c * K, K), K), :], pool.at[lobby(c)], f_sem.at[c])

    def flip(n, c):
        pool[lax.rem(n, 2), :, pl.ds(aligned(c * K, K), K)] = a_in[lax.rem(c, 4)].T

    def swap(i):
        return remote(give, take.at[lax.rem(i, 3)], d_send.at[0], d_recv.at[lax.rem(i, 3)], other)

    def scatter(v, s):
        src, dst = ((s1, r1), (s2, r2), (s3, r3))[s]
        _, to = route(v, s)
        q = lax.rem(v, 6)
        return remote(src.at[lax.rem(v, 3)], dst.at[q], rs_send.at[s, lax.rem(v, 3)], rs_recv.at[s, q], to)

    def start_of(v, s):
        row, size = core * half, half
        for k in range(s):
            size //= 2
            row = row + route(v, k)[0] * size
        return row, size

    def gather(v, s):
        row, size = start_of(v, s + 1)
        _, to = route(v, s)
        q = lax.rem(v, 12)
        ref = pool.at[spot(v, aligned(row, rows // 16), size)]
        return remote(ref, ref, ag_send.at[s, q], ag_recv.at[s, q], to)

    def share(v):
        q = lax.rem(v, 12)
        ref = pool.at[spot(v, aligned(core * half, half), half)]
        return remote(ref, ref, ag_send.at[3, q], ag_recv.at[3, q], other)

    def add(v, s, mine, got, keep, send):
        bit, _ = route(v, s)
        n = got.shape[0] // 2
        yes, no = pl.ds(aligned(bit * n, n), n), pl.ds(aligned((1 - bit) * n, n), n)
        q = lax.rem(v, 3)
        send[q] = (mine[no, :] + got[no, :].astype(jnp.float32)).astype(jnp.bfloat16)
        keep[q] = mine[yes, :] + got[yes, :].astype(jnp.float32)

    def stages(t, h):
        def when(k, f):
            v = t - LAG[k]
            pl.when((v >= 0) & (v < units))(lambda: f(v))

        def nine(v):
            pl.when(v < early)(lambda: o_copy(v).wait())

        def eight(v):
            share(v).wait()
            pl.when(v < early)(lambda: o_copy(v).start())

        def seven(v):
            gather(v, 0).wait()
            share(v).start()

        def six(v):
            gather(v, 1).wait()
            gather(v, 0).start()

        def five(v):
            gather(v, 2).wait()
            gather(v, 1).start()

        def four(v):
            scatter(v, 2).wait()
            row, size = start_of(v, 3)
            done = keep3[lax.rem(v, 3)] + r3[lax.rem(v, 6)].astype(jnp.float32)
            pool[spot(v, aligned(row, rows // 16), size)] = done.astype(jnp.bfloat16)
            gather(v, 2).start()

        def three(v):
            scatter(v, 1).wait()
            add(v, 2, keep2.at[lax.rem(v, 3)], r2.at[lax.rem(v, 6)], keep3, s3)
            scatter(v, 2).start()

        def two(v):
            scatter(v, 0).wait()
            add(v, 1, keep1.at[lax.rem(v, 3)], r1.at[lax.rem(v, 6)], keep2, s2)
            scatter(v, 1).start()

        def one(v):
            p = (h - LAG[1]) % 2
            i = v // 2
            if p == 0:
                swap(i).wait()
            c = slice(p * W, (p + 1) * W)
            add(v, 0, acc.at[:, c], take.at[lax.rem(i, 3), :, c], keep1, s1)
            scatter(v, 0).start()

        for k, f in enumerate((one, two, three, four, five, six, seven, eight, nine), 1):
            when(k, f)

    lax.fori_loop(0, chunks, lambda c, _: (a_first(c).start(), 0)[1], 0)
    for c in g_copies(0):
        c.start()
    barrier = pltpu.get_barrier_semaphore()
    for b, bit in ((8, bits[0]), (4, bits[1]), (2, bits[2]), (1, core)):
        pl.semaphore_signal(barrier, inc=1, device_id={"dp": me + b * (1 - 2 * bit)}, device_id_type=MESH)
    pl.semaphore_wait(barrier, 4)

    def first(c, _):
        a_first(c).wait()
        pool[0, :, pl.ds(aligned(c * K, K), K)] = pool[lobby(c)].T
        return 0

    lax.fori_loop(0, chunks, first, 0)

    def pair(i, _):
        n = (2 * i) // per
        for h in range(2):
            t = 2 * i + h
            c = 2 * (lax.rem(t, per) - (per - chunks // 2))
            ahead = (t < units - per) & (c >= 0)

            @pl.when(ahead)
            def _():
                a_copy(n + 1, c).start()
                a_copy(n + 1, c + 1).start()

            stages(t, h)
            fetch(t - 3, lambda c: c.wait())
            fetch(t, lambda c: c.start())

            @pl.when(t < units)
            def _():
                if h == 0:
                    for c_ in g_copies(i):
                        c_.wait()

                    @pl.when(i + 1 < units // 2)
                    def _():
                        for c_ in g_copies(i + 1):
                            c_.start()
                side = core if h else 1 - core
                mine = lax.rem(n, 2), pl.ds(aligned(side * half, half), half)
                block = sum(jnp.dot(pool[(*mine, pl.ds(q * deep, deep))], pool[piece(i, q)], preferred_element_type=jnp.float32)
                            for q in range(4))
                if h == 0:
                    give[...] = block.astype(jnp.bfloat16)
                    swap(i).start()
                else:
                    acc[...] = block

            @pl.when(ahead)
            def _():
                for q in range(2):
                    a_copy(n + 1, c + q).wait()
                    flip(n + 1, c + q)
        return 0

    lax.fori_loop(0, (units + LAG[9] + 1 + 1) // 2, pair, 0)


def settle(shape, pool, out, sem):
    mats, rows, cols = shape
    per = cols // W
    units = mats * per
    copies, f = [], 0
    while f < units:
        n = min(LANES - f % LANES, per - f % per)
        b = f // LANES if f < units - SPARE else UNITS + f % SPARE // LANES
        for r in range(0, rows, rows // ROWS):
            part = pl.ds(r, rows // ROWS)
            copies.append(pltpu.make_async_copy(pool.at[b, part, pl.ds(f % LANES * W, n * W)],
                                                out.at[f // per, part, pl.ds(f % per * W, n * W)], sem.at[len(copies)]))
        f += n
    for c in copies:
        c.start()
    for c in copies:
        c.wait()


def solution(mesh):
    def step(a, g):
        _, mats, tokens, rows = a.shape
        cols = g.shape[3]
        half = rows // 2
        bf, f32 = jnp.bfloat16, jnp.float32
        dma = pltpu.SemaphoreType.DMA
        _, pool = pl.pallas_call(
            lambda *refs: kernel((mats, tokens, rows, cols), *refs),
            out_shape=(jax.ShapeDtypeStruct((mats, rows, cols), bf), pltpu.VMEM((BLOCKS, rows, LANES * W), bf)),
            in_specs=[pl.BlockSpec(memory_space=pl.ANY)] * 2,
            out_specs=(pl.BlockSpec(memory_space=pl.ANY), pl.BlockSpec(memory_space=pltpu.VMEM)),
            scratch_shapes=[
                pltpu.VMEM((4, K, rows), bf),
                pltpu.VMEM((half, 2 * W), f32),
                pltpu.VMEM((half, 2 * W), bf),
                pltpu.VMEM((3, half, 2 * W), bf),
                *[pltpu.VMEM((3, half // d, W), f32) for d in (2, 4, 8)],
                *[pltpu.VMEM((3, half // d, W), bf) for d in (2, 4, 8)],
                *[pltpu.VMEM((6, half // d, W), bf) for d in (2, 4, 8)],
                dma((4,)), dma((tokens // K,)), dma((2, 4)), dma((3,)), dma((8,)), dma((1,)), dma((3,)),
                dma((3, 3)), dma((3, 6)), dma((4, 12)), dma((4, 12)),
            ],
            compiler_params=pltpu.CompilerParams(collective_id=0, has_side_effects=True, vmem_limit_bytes=14417920),
        )(a, g)
        return pl.pallas_call(
            lambda *refs: settle((mats, rows, cols), *refs),
            out_shape=jax.ShapeDtypeStruct((mats, rows, cols), bf),
            in_specs=[pl.BlockSpec(memory_space=pltpu.VMEM)],
            out_specs=pl.BlockSpec(memory_space=pl.ANY),
            scratch_shapes=[dma((8 * ROWS,))],
            compiler_params=pltpu.CompilerParams(vmem_limit_bytes=2**20),
        )(pool)

    return jax.shard_map(step, mesh=mesh, in_specs=(P(("rep", "dp")), P(("rep", "dp"))), out_specs=P("rep"), check_vma=False)
```
